32 devices in a mesh: band: 8 (over z, x), ga: 4 (over y, core).
Axes of the slice: x: 2, y: 2, z: 4, core: 2. Of those that a mesh axis runs over, the one named last changes fastest.
Arguments:
- elements: bfloat16 [2, 768, 2048], P(None, 'band', 'ga'), may hold values from -0.75 to 0.75
- screened: bfloat16 [2, 2, 2048, 2048], P(None, None, 'ga'), may hold values from -0.09375 to 0.09375
- energies: float32 [768], replicated, may hold values from -3 to 3
- freq_points: float32 [2], replicated, may hold values from -3 to 3
- freq_weights: float32 [2], replicated, may hold values from 0.5 to 2
- band_of_slot: int32 [768], replicated, may hold values from 0 to 767, each once
Outputs:
- sigma: float32 [2, 768, 768], P(None, 'band', 'ga')
The draws below stay inside these ranges and needn't reach their ends.
Inputs may be any that keep to these rules, and one draw needn't show every extreme that they name: `band_of_slot`: each of 0 to 767 stands once.
All inputs are finite; a program needn't handle non-finite values.
Results may differ from the reference program's by a relative error of at most 0.0042.
Values may be sent and summed in bfloat16 or wider, within the bound.
No kernel may reach another device: no remote copies, remote signals or barrier semaphores. Data moves between devices by JAX's collectives and lax.ppermute only.
A program may use at most 128 MiB of HBM per device.

```python
import math
import jax
import jax.numpy as jnp

NG = 2048
NW = 2
NB = 768


def block_levels(rng, extent, split, smallest, high):
    gain = 1.0
    for axis_at, blocks in split:
        heights = jax.random.uniform(jax.random.fold_in(jax.random.fold_in(rng, 6), axis_at), (blocks,), jnp.float32, smallest / len(split), high / len(split))
        gain = gain * jnp.repeat(jnp.exp(heights), extent[axis_at] // blocks).reshape((-1,) + (1,) * (len(extent) - 1 - axis_at))
    return gain


def normal_values(rng, dims, deviation, limit, shards=(), dtype=jnp.bfloat16):
    values = deviation * jax.random.normal(rng, dims, jnp.float32)
    if shards:
        values = values * block_levels(rng, dims, shards, -0.22, 0.18)
    return jnp.clip(values, -limit, limit).astype(dtype)


def setup_inputs(seed: int = 0) -> dict:
    keys = jax.random.split(jax.random.key(seed), 7)
    elements = normal_values(keys[0], (2, NB, NG), 0.125, 0.75, ((1, 8), (2, 4)))
    screened = normal_values(keys[1], (NW, 2, NG, NG), (2 * NG) ** -0.5, 0.09375, ((2, 4),))
    energies = jnp.clip(jax.random.uniform(keys[2], (NB,), jnp.float32, -3.0, 3.0), -3.0, 3.0)
    freq_points = jnp.clip(jax.random.uniform(keys[3], (NW,), jnp.float32, -3.0, 3.0), -3.0, 3.0)
    freq_weights = jnp.clip(jnp.exp(jax.random.uniform(keys[4], (NW,), jnp.float32, math.log(0.5), math.log(2.0))), 0.5, 2.0)
    band_of_slot = jax.random.permutation(keys[5], NB).astype(jnp.int32)
    return dict(elements=elements, screened=screened, energies=energies, freq_points=freq_points, freq_weights=freq_weights, band_of_slot=band_of_slot)


def reference(elements, screened, energies, freq_points, freq_weights, band_of_slot):
    slot_energy = jnp.take(energies, band_of_slot.astype(jnp.int32))
    offset = slot_energy[None, :] - freq_points[:, None]
    screen = freq_weights[:, None] / (1.0 + 4.0 * offset * offset)
    real_part = elements[0]
    imag_part = elements[1]
    total = jnp.zeros((2, NB, NB), jnp.float32)
    for freq in range(NW):
        w_real = screened[freq, 0]
        w_imag = screened[freq, 1]
        y_real = (jnp.dot(real_part, w_real.T, preferred_element_type=jnp.float32)
                  - jnp.dot(imag_part, w_imag.T, preferred_element_type=jnp.float32)).astype(jnp.bfloat16)
        y_imag = (jnp.dot(real_part, w_imag.T, preferred_element_type=jnp.float32)
                  + jnp.dot(imag_part, w_real.T, preferred_element_type=jnp.float32)).astype(jnp.bfloat16)
        pair_real = (jnp.dot(real_part, y_real.T, preferred_element_type=jnp.float32)
                     + jnp.dot(imag_part, y_imag.T, preferred_element_type=jnp.float32))
        pair_imag = (jnp.dot(real_part, y_imag.T, preferred_element_type=jnp.float32)
                     - jnp.dot(imag_part, y_real.T, preferred_element_type=jnp.float32))
        factor = 0.5 * (screen[freq][:, None] + screen[freq][None, :])
        total = total + factor[None] * jnp.stack([pair_real, pair_imag])
    return total
```

```python
import jax
import jax.numpy as jnp
from jax import lax
from jax.sharding import PartitionSpec as P

BOTH = ("band", "ga")


def build(B, A):
    R = B // A

    def move(value, step):
        pairs = []
        for row in range(A):
            for r in range(R):
                for a in range(A):
                    to = step(row, r, a)
                    if to is not None:
                        pairs.append(((row * R + r) * A + a, (to[0] * R + to[1]) * A + to[2]))
        return lax.ppermute(value, BOTH, pairs)

    def down(row, r, a):
        return (row + 1, r, a) if row + 1 < A else None

    def up(row, r, a):
        return (row - 1, r, a) if row > 0 else None

    def flip(bit):
        return lambda row, r, a: (row, r, a ^ bit)

    def turn(offset):
        return lambda row, r, a: (row, (r - offset) % R, a)

    def on_device(elements, screened, energies, freq_points, freq_weights, band_of_slot):
        bands = elements.shape[1]
        band = lax.axis_index("band")
        row, r = band // R, band % R
        a = lax.axis_index("ga")

        high = A // 2
        across = move(elements, flip(high))
        beside = [move(elements, turn(o)) for o in range(1, R)]
        lower, upper = [None], [None]
        lower.append(move(elements, down))
        upper.append(move(elements, up))
        both = [
            jnp.stack([move(piece[0], flip(high)), move(across[1], turn(o))])
            for o, piece in zip(range(1, R), beside)
        ]
        mine = jnp.concatenate([elements] + beside, axis=1)
        far = jnp.concatenate([across] + both, axis=1)
        known = {0: mine, high: far}
        bit = high // 2
        while bit:
            for j in list(known):
                known[j | bit] = move(known[j], flip(bit))
            bit //= 2
        for k in range(2, A):
            lower.append(move(lower[-1], down))
            upper.append(move(upper[-1], up))

        relative = jnp.stack([known[j] for j in range(A)])
        piece = jnp.concatenate(
            [lax.dynamic_index_in_dim(relative, j ^ a, 0, keepdims=False) for j in range(A)], axis=2
        )
        sides = jnp.stack([jnp.stack([piece[0], -piece[1]]), jnp.stack([piece[1], piece[0]])])
        applied = jnp.einsum(
            "dcmk,wcgk->wdmg", sides, screened, preferred_element_type=jnp.float32
        ).astype(jnp.bfloat16)

        at = [elements] + [jnp.where(row + o < A, upper[o], lower[A - o]) for o in range(1, A)]
        at = jnp.stack(at)
        turned = [lax.dynamic_index_in_dim(at, (a + k - row) % A, 0, keepdims=False) for k in range(A)]

        slot_energy = jnp.take(energies, band_of_slot)
        offset = slot_energy[None, :] - freq_points[:, None]
        screen = freq_weights[:, None] / (1.0 + 4.0 * offset * offset)

        def screen_of(row_at, r_at):
            return lax.dynamic_slice_in_dim(screen, (row_at * R + r_at) * bands, bands, 1)

        right = jnp.concatenate([screen_of(row, (r + o) % R) for o in range(R)], axis=1)
        parts = []
        for k in range(A):
            block = turned[k]
            left = jnp.stack([block, jnp.stack([-block[1], block[0]])])
            pairs = jnp.einsum(
                "dcnk,wcmk->wdnm", left, applied, preferred_element_type=jnp.float32
            )
            factor = 0.5 * (screen_of((a + k) % A, r)[:, :, None] + right[:, None, :])
            parts.append(jnp.sum(pairs * factor[:, None], axis=0).astype(jnp.bfloat16))
        got = [
            move(parts[k], lambda row, r, a, k=k: ((a + k) % A, r, row)) for k in range(A)
        ]
        total = got[0].astype(jnp.float32)
        for part in got[1:]:
            total = total + part.astype(jnp.float32)
        cut = jnp.split(total, R, axis=2)
        if R == 1:
            return total
        cut = jnp.stack(cut)
        return jnp.concatenate(
            [lax.dynamic_index_in_dim(cut, (j - r) % R, 0, keepdims=False) for j in range(R)], axis=2
        )

    return on_device


def solution(mesh):
    placed = (P(None, "band", "ga"), P(None, None, "ga", None), P(), P(), P(), P())
    return jax.shard_map(
        build(mesh.shape["band"], mesh.shape["ga"]),
        mesh=mesh, in_specs=placed, out_specs=P(None, "band", "ga"), check_vma=False
    )
```

```python
import jax
import jax.numpy as jnp
from jax import lax
from jax.sharding import PartitionSpec as P


BOTH = ("band", "ga")


def build(B, A):
    R = B // A

    def move(value, step):
        pairs = []
        for row in range(A):
            for r in range(R):
                for a in range(A):
                    to = step(row, r, a)
                    if to is not None:
                        pairs.append(((row * R + r) * A + a, (to[0] * R + to[1]) * A + to[2]))
        return lax.ppermute(value, BOTH, pairs)

    def swap(offset):
        return lambda row, r, a: (row ^ offset, r, a)

    def transpose(row, r, a):
        return (a, r, row)

    def flip(bit):
        return lambda row, r, a: (row, r, a ^ bit)

    def turn(offset):
        return lambda row, r, a: (row, (r - offset) % R, a)

    def on_device(elements, screened, energies, freq_points, freq_weights, band_of_slot):
        bands = elements.shape[1]
        band = lax.axis_index("band")
        row, r = band // R, band % R
        a = lax.axis_index("ga")

        high = A // 2
        across = move(elements, flip(high))
        beside = [move(elements, turn(o)) for o in range(1, R)]
        at = [elements]
        for o in range(1, A):
            at.append(move(elements, swap(o)))
        both = [
            jnp.stack([move(piece[0], flip(high)), move(across[1], turn(o))])
            for o, piece in zip(range(1, R), beside)
        ]
        mine = jnp.concatenate([elements] + beside, axis=1)
        far = jnp.concatenate([across] + both, axis=1)
        known = {0: mine, high: far}
        bit = high // 2
        while bit:
            for j in list(known):
                known[j | bit] = move(known[j], flip(bit))
            bit //= 2
        relative = jnp.stack([known[j] for j in range(A)])
        piece = jnp.concatenate(
            [lax.dynamic_index_in_dim(relative, j ^ a, 0, keepdims=False) for j in range(A)], axis=2
        )
        sides = jnp.stack([jnp.stack([piece[0], -piece[1]]), jnp.stack([piece[1], piece[0]])])
        applied = jnp.einsum(
            "dcmk,wcgk->wdmg", sides, screened, preferred_element_type=jnp.float32
        ).astype(jnp.bfloat16)

        at = jnp.stack(at)
        turned = [lax.dynamic_index_in_dim(at, row ^ a ^ j, 0, keepdims=False) for j in range(A)]

        band_of_slot, _ = lax.optimization_barrier((band_of_slot, far))
        slot_energy = jnp.take(energies, band_of_slot)
        offset = slot_energy[None, :] - freq_points[:, None]
        screen = freq_weights[:, None] / (1.0 + 4.0 * offset * offset)

        def screen_of(row_at, r_at):
            return lax.dynamic_slice_in_dim(screen, (row_at * R + r_at) * bands, bands, 1)

        right = jnp.concatenate([screen_of(row, (r + o) % R) for o in range(R)], axis=1)
        parts = {}
        for j in reversed(range(A)):
            block = turned[j]
            left = jnp.stack([block, jnp.stack([-block[1], block[0]])])
            pairs = jnp.einsum(
                "dcnk,wcmk->wdnm", left, applied, preferred_element_type=jnp.float32
            )
            factor = 0.5 * (screen_of(a ^ j, r)[:, :, None] + right[:, None, :])
            parts[j] = jnp.sum(pairs * factor[:, None], axis=0)
        bit = 1
        while bit < A:
            wire = jnp.float32 if bit < high else jnp.bfloat16
            kept = [j for j in parts if not j & bit]
            sent = jnp.stack([parts[j | bit].astype(wire) for j in kept])
            got = move(sent, flip(bit)).astype(jnp.float32)
            parts = {j: parts[j] + got[i] for i, j in enumerate(kept)}
            bit *= 2
        total = move(parts[0].astype(jnp.bfloat16), transpose).astype(jnp.float32)
        cut = jnp.split(total, R, axis=2)
        if R == 1:
            return total
        cut = jnp.stack(cut)
        return jnp.concatenate(
            [lax.dynamic_index_in_dim(cut, (j - r) % R, 0, keepdims=False) for j in range(R)], axis=2
        )

    return on_device


def solution(mesh):
    placed = (P(None, "band", "ga"), P(None, None, "ga", None), P(), P(), P(), P())
    A = mesh.shape["ga"]
    body = build(mesh.shape["band"], A)

    return jax.shard_map(
        body, mesh=mesh, in_specs=placed, out_specs=P(None, "band", "ga"), check_vma=False
    )
```

```python
import jax
import jax.numpy as jnp
from jax import lax
from jax.experimental import pallas as pl
from jax.experimental.pallas import tpu as pltpu
from jax.sharding import PartitionSpec as P


BOTH = ("band", "ga")


def apply_screened(order, pieces, screened):
    count = len(pieces)
    _, m, k = pieces[0].shape
    freqs, _, g, total = screened.shape
    tile = min(g, 256)

    def kernel(order_ref, *refs):
        piece_refs, w_ref, out_ref = refs[:count], refs[count], refs[count + 1]
        real, imag, minus = refs[count + 2:]

        @pl.when((pl.program_id(0) == 0) & (pl.program_id(1) == 0))
        def _():
            for j in range(count):
                columns = pl.ds(pl.multiple_of(order_ref[j] * k, k), k)
                real[:, columns] = piece_refs[j][0]
                imag[:, columns] = piece_refs[j][1]
                minus[:, columns] = -piece_refs[j][1]

        def dot(left, right):
            return lax.dot_general(
                left, right, (((1,), (1,)), ((), ())), preferred_element_type=jnp.float32
            )

        first = dot(real[...], w_ref[0, 0]) + dot(minus[...], w_ref[0, 1])
        out_ref[0, 0] = first.astype(jnp.bfloat16)
        second = dot(imag[...], w_ref[0, 0]) + dot(real[...], w_ref[0, 1])
        out_ref[0, 1] = second.astype(jnp.bfloat16)

    whole = pl.BlockSpec((2, m, k), lambda w, t, order_ref: (0, 0, 0))
    return pl.pallas_call(
        kernel,
        grid_spec=pltpu.PrefetchScalarGridSpec(
            num_scalar_prefetch=1,
            grid=(freqs, g // tile),
            in_specs=[whole] * count
            + [pl.BlockSpec((1, 2, tile, total), lambda w, t, order_ref: (w, 0, t, 0))],
            out_specs=pl.BlockSpec((1, 2, m, tile), lambda w, t, order_ref: (w, 0, 0, t)),
            scratch_shapes=[pltpu.VMEM((m, total), jnp.bfloat16)] * 3,
        ),
        out_shape=jax.ShapeDtypeStruct((freqs, 2, m, g), jnp.bfloat16),
        compiler_params=pltpu.CompilerParams(vmem_limit_bytes=40 * 2**20),
        cost_estimate=pl.CostEstimate(
            flops=8 * freqs * m * g * total,
            bytes_accessed=2 * screened.size + 4 * freqs * m * g + 4 * m * total,
            transcendentals=0,
        ),
    )(order, *pieces, screened)


def small(R):
    return R <= 4


def build(B, A):
    R = B // A

    def move(value, step):
        pairs = []
        for row in range(A):
            for r in range(R):
                for a in range(A):
                    to = step(row, r, a)
                    if to is not None:
                        pairs.append(((row * R + r) * A + a, (to[0] * R + to[1]) * A + to[2]))
        return lax.ppermute(value, BOTH, pairs)

    def swap(offset):
        return lambda row, r, a: (row ^ offset, r, a)

    def transpose(row, r, a):
        return (a, r, row)

    def flip(bit):
        return lambda row, r, a: (row, r, a ^ bit)

    def turn(offset):
        return lambda row, r, a: (row, (r - offset) % R, a)

    def on_device(elements, screened, energies, freq_points, freq_weights, band_of_slot):
        bands = elements.shape[1]
        band = lax.axis_index("band")
        row, r = band // R, band % R
        a = lax.axis_index("ga")

        high = A // 2
        across = move(elements, flip(high))
        beside = [move(elements, turn(o)) for o in range(1, R)]
        at = [elements]
        for o in range(1, A):
            at.append(move(elements, swap(o)))
        both = [
            jnp.stack([move(piece[0], flip(high)), move(across[1], turn(o))])
            for o, piece in zip(range(1, R), beside)
        ]
        mine = jnp.concatenate([elements] + beside, axis=1)
        far = jnp.concatenate([across] + both, axis=1)
        known = {0: mine, high: far}
        bit = high // 2
        while bit:
            for j in list(known):
                known[j | bit] = move(known[j], flip(bit))
            bit //= 2
        if small(R):
            order = jnp.stack([a ^ j for j in range(A)]).astype(jnp.int32)
            applied = apply_screened(order, [known[j] for j in range(A)], screened)
        else:
            relative = jnp.stack([known[j] for j in range(A)])
            piece = jnp.concatenate(
                [lax.dynamic_index_in_dim(relative, j ^ a, 0, keepdims=False) for j in range(A)],
                axis=2,
            )
            sides = jnp.stack([jnp.stack([piece[0], -piece[1]]), jnp.stack([piece[1], piece[0]])])
            applied = jnp.einsum(
                "dcmk,wcgk->wdmg", sides, screened, preferred_element_type=jnp.float32
            ).astype(jnp.bfloat16)

        at = jnp.stack(at)
        turned = [lax.dynamic_index_in_dim(at, row ^ a ^ j, 0, keepdims=False) for j in range(A)]

        if small(R):
            hit = band_of_slot[None, :] == lax.iota(jnp.int32, energies.shape[0])[:, None]
            slot_energy = jnp.sum(jnp.where(hit, energies[:, None], 0.0), axis=0)
        else:
            slot_energy = jnp.take(energies, band_of_slot)
        offset = slot_energy[None, :] - freq_points[:, None]
        screen = freq_weights[:, None] / (1.0 + 4.0 * offset * offset)

        def screen_of(row_at, r_at):
            return lax.dynamic_slice_in_dim(screen, (row_at * R + r_at) * bands, bands, 1)

        right = jnp.concatenate([screen_of(row, (r + o) % R) for o in range(R)], axis=1)
        parts = {}
        for j in reversed(range(A)):
            block = turned[j]
            left = jnp.stack([block, jnp.stack([-block[1], block[0]])])
            pairs = jnp.einsum(
                "dcnk,wcmk->wdnm", left, applied, preferred_element_type=jnp.float32
            )
            factor = 0.5 * (screen_of(a ^ j, r)[:, :, None] + right[:, None, :])
            parts[j] = jnp.sum(pairs * factor[:, None], axis=0)
        bit = 1
        while bit < A:
            wire = jnp.float32 if bit < high else jnp.bfloat16
            kept = [j for j in parts if not j & bit]
            sent = jnp.stack([parts[j | bit].astype(wire) for j in kept])
            got = move(sent, flip(bit)).astype(jnp.float32)
            parts = {j: parts[j] + got[i] for i, j in enumerate(kept)}
            bit *= 2
        total = move(parts[0].astype(jnp.bfloat16), transpose).astype(jnp.float32)
        cut = jnp.split(total, R, axis=2)
        if R == 1:
            return total
        cut = jnp.stack(cut)
        return jnp.concatenate(
            [lax.dynamic_index_in_dim(cut, (j - r) % R, 0, keepdims=False) for j in range(R)], axis=2
        )

    return on_device


def solution(mesh):
    placed = (P(None, "band", "ga"), P(None, None, "ga", None), P(), P(), P(), P())
    A = mesh.shape["ga"]
    body = build(mesh.shape["band"], A)

    return jax.shard_map(
        body, mesh=mesh, in_specs=placed, out_specs=P(None, "band", "ga"), check_vma=False
    )
```

```python
import jax
import jax.numpy as jnp
from jax import lax
from jax.experimental import pallas as pl
from jax.experimental.pallas import tpu as pltpu
from jax.sharding import PartitionSpec as P


BOTH = ("band", "ga")


def apply_screened(order, pieces, screened):
    count = len(pieces)
    _, m, k = pieces[0].shape
    freqs, _, g, total = screened.shape
    tile = min(g, 256)
    steps = [(w, t) for w in range(freqs) for t in range(0, g, tile)]

    def kernel(order_ref, *refs):
        piece_refs, w_hbm, out_ref = refs[:count], refs[count], refs[count + 1]
        w_ref, real, imag, minus, sems = refs[count + 2:]
        copies = [
            pltpu.make_async_copy(
                w_hbm.at[w, :, pl.ds(t, tile), :], w_ref.at[i], sems.at[i]
            )
            for i, (w, t) in enumerate(steps)
        ]
        for copy in copies:
            copy.start()
        for j in range(count):
            columns = pl.ds(pl.multiple_of(order_ref[j] * k, k), k)
            real[:, columns] = piece_refs[j][0]
            imag[:, columns] = piece_refs[j][1]
            minus[:, columns] = -piece_refs[j][1]

        def dot(left, right):
            return lax.dot_general(
                left, right, (((1,), (1,)), ((), ())), preferred_element_type=jnp.float32
            )

        for i, (w, t) in enumerate(steps):
            copies[i].wait()
            first = dot(real[...], w_ref[i, 0]) + dot(minus[...], w_ref[i, 1])
            out_ref[w, 0, :, pl.ds(t, tile)] = first.astype(jnp.bfloat16)
            second = dot(imag[...], w_ref[i, 0]) + dot(real[...], w_ref[i, 1])
            out_ref[w, 1, :, pl.ds(t, tile)] = second.astype(jnp.bfloat16)

    in_vmem = pl.BlockSpec(memory_space=pltpu.VMEM)
    return pl.pallas_call(
        kernel,
        in_specs=[pl.BlockSpec(memory_space=pltpu.SMEM)]
        + [in_vmem] * count
        + [pl.BlockSpec(memory_space=pltpu.HBM)],
        out_specs=in_vmem,
        scratch_shapes=[pltpu.VMEM((len(steps), 2, tile, total), jnp.bfloat16)]
        + [pltpu.VMEM((m, total), jnp.bfloat16)] * 3
        + [pltpu.SemaphoreType.DMA((len(steps),))],
        out_shape=jax.ShapeDtypeStruct((freqs, 2, m, g), jnp.bfloat16),
        compiler_params=pltpu.CompilerParams(vmem_limit_bytes=57 * 2**20),
        cost_estimate=pl.CostEstimate(
            flops=8 * freqs * m * g * total,
            bytes_accessed=2 * screened.size + 4 * freqs * m * g + 4 * m * total,
            transcendentals=0,
        ),
    )(order, *pieces, screened)


def small(R):
    return R <= 4


def build(B, A):
    R = B // A

    def move(value, step):
        pairs = []
        for row in range(A):
            for r in range(R):
                for a in range(A):
                    to = step(row, r, a)
                    if to is not None:
                        pairs.append(((row * R + r) * A + a, (to[0] * R + to[1]) * A + to[2]))
        return lax.ppermute(value, BOTH, pairs)

    def swap(offset):
        return lambda row, r, a: (row ^ offset, r, a)

    def transpose(row, r, a):
        return (a, r, row)

    def flip(bit):
        return lambda row, r, a: (row, r, a ^ bit)

    def turn(offset):
        return lambda row, r, a: (row, (r - offset) % R, a)

    def on_device(elements, screened, energies, freq_points, freq_weights, band_of_slot):
        bands = elements.shape[1]
        band = lax.axis_index("band")
        row, r = band // R, band % R
        a = lax.axis_index("ga")

        high = A // 2
        across = move(elements, flip(high))
        beside = [move(elements, turn(o)) for o in range(1, R)]
        at = [elements]
        for o in range(1, A):
            at.append(move(elements, swap(o)))
        both = []
        for o, piece in zip(range(1, R), beside):
            one = move(piece[0], flip(high))
            both.append(jnp.stack([one, move(across[1], turn(o))]))
        mine = jnp.concatenate([elements] + beside, axis=1)
        far = jnp.concatenate([across] + both, axis=1)
        known = {0: mine, high: far}
        bit = high // 2
        while bit:
            for j in list(known):
                known[j | bit] = move(known[j], flip(bit))
            bit //= 2
        if small(R):
            order = jnp.stack([a ^ j for j in range(A)]).astype(jnp.int32)
            applied = apply_screened(order, [known[j] for j in range(A)], screened)
        else:
            relative = jnp.stack([known[j] for j in range(A)])
            piece = jnp.concatenate(
                [lax.dynamic_index_in_dim(relative, j ^ a, 0, keepdims=False) for j in range(A)],
                axis=2,
            )
            sides = jnp.stack([jnp.stack([piece[0], -piece[1]]), jnp.stack([piece[1], piece[0]])])
            applied = jnp.einsum(
                "dcmk,wcgk->wdmg", sides, screened, preferred_element_type=jnp.float32
            ).astype(jnp.bfloat16)

        at = jnp.stack(at)
        turned = [lax.dynamic_index_in_dim(at, row ^ a ^ j, 0, keepdims=False) for j in range(A)]

        band_of_slot, energies, _ = lax.optimization_barrier((band_of_slot, energies, far))
        if small(R):
            hit = band_of_slot[None, :] == lax.iota(jnp.int32, energies.shape[0])[:, None]
            slot_energy = jnp.sum(jnp.where(hit, energies[:, None], 0.0), axis=0)
        else:
            slot_energy = jnp.take(energies, band_of_slot)
        offset = slot_energy[None, :] - freq_points[:, None]
        screen = freq_weights[:, None] / (1.0 + 4.0 * offset * offset)

        def screen_of(row_at, r_at):
            return lax.dynamic_slice_in_dim(screen, (row_at * R + r_at) * bands, bands, 1)

        right = jnp.concatenate([screen_of(row, (r + o) % R) for o in range(R)], axis=1)
        parts = {}
        for j in reversed(range(A)):
            block = turned[j]
            left = jnp.stack([block, jnp.stack([-block[1], block[0]])])
            pairs = jnp.einsum(
                "dcnk,wcmk->wdnm", left, applied, preferred_element_type=jnp.float32
            )
            factor = 0.5 * (screen_of(a ^ j, r)[:, :, None] + right[:, None, :])
            parts[j] = jnp.sum(pairs * factor[:, None], axis=0)
        bit = 1
        while bit < A:
            wire = jnp.float32 if bit < high else jnp.bfloat16
            kept = [j for j in parts if not j & bit]
            sent = jnp.stack([parts[j | bit].astype(wire) for j in kept])
            got = move(sent, flip(bit)).astype(jnp.float32)
            parts = {j: parts[j] + got[i] for i, j in enumerate(kept)}
            bit *= 2
        total = move(parts[0].astype(jnp.bfloat16), transpose).astype(jnp.float32)
        cut = jnp.split(total, R, axis=2)
        if R == 1:
            return total
        cut = jnp.stack(cut)
        return jnp.concatenate(
            [lax.dynamic_index_in_dim(cut, (j - r) % R, 0, keepdims=False) for j in range(R)], axis=2
        )

    return on_device


def solution(mesh):
    placed = (P(None, "band", "ga"), P(None, None, "ga", None), P(), P(), P(), P())
    A = mesh.shape["ga"]
    body = build(mesh.shape["band"], A)

    return jax.shard_map(
        body, mesh=mesh, in_specs=placed, out_specs=P(None, "band", "ga"), check_vma=False
    )
```

```python
import jax
import jax.numpy as jnp
from jax import lax
from jax.sharding import PartitionSpec as P


BOTH = ("band", "ga")


def build(B, A):
    R = B // A

    def move(value, step):
        pairs = []
        for row in range(A):
            for r in range(R):
                for a in range(A):
                    to = step(row, r, a)
                    if to is not None:
                        pairs.append(((row * R + r) * A + a, (to[0] * R + to[1]) * A + to[2]))
        return lax.ppermute(value, BOTH, pairs)

    def swap(offset):
        return lambda row, r, a: (row ^ offset, r, a)

    def transpose(row, r, a):
        return (a, r, row)

    def flip(bit):
        return lambda row, r, a: (row, r, a ^ bit)

    def turn(offset):
        return lambda row, r, a: (row, (r - offset) % R, a)

    def on_device(elements, screened, energies, freq_points, freq_weights, band_of_slot):
        bands = elements.shape[1]
        band = lax.axis_index("band")
        row, r = band // R, band % R
        a = lax.axis_index("ga")

        high = A // 2
        across = move(elements, flip(high))
        beside = [move(elements, turn(o)) for o in range(1, R)]
        at = [elements]
        for o in range(1, A):
            at.append(move(elements, swap(o)))
        both = []
        for o, piece in zip(range(1, R), beside):
            one = move(piece[0], flip(high))
            both.append(jnp.stack([one, move(across[1], turn(o))]))
        mine = jnp.concatenate([elements] + beside, axis=1)
        far = jnp.concatenate([across] + both, axis=1)
        known = {0: mine, high: far}
        bit = high // 2
        while bit:
            for j in list(known):
                known[j | bit] = move(known[j], flip(bit))
            bit //= 2
        relative = jnp.stack([known[j] for j in range(A)])
        piece = jnp.concatenate(
            [lax.dynamic_index_in_dim(relative, j ^ a, 0, keepdims=False) for j in range(A)], axis=2
        )
        sides = jnp.stack([jnp.stack([piece[0], -piece[1]]), jnp.stack([piece[1], piece[0]])])
        applied = jnp.einsum(
            "dcmk,wcgk->wdmg", sides, screened, preferred_element_type=jnp.float32
        ).astype(jnp.bfloat16)

        at = jnp.stack(at)
        turned = [lax.dynamic_index_in_dim(at, row ^ a ^ j, 0, keepdims=False) for j in range(A)]

        band_of_slot, energies, _ = lax.optimization_barrier((band_of_slot, energies, far))
        if R <= 4:
            hit = band_of_slot[None, :] == lax.iota(jnp.int32, energies.shape[0])[:, None]
            slot_energy = jnp.sum(jnp.where(hit, energies[:, None], 0.0), axis=0)
        else:
            slot_energy = jnp.take(energies, band_of_slot)
        offset = slot_energy[None, :] - freq_points[:, None]
        screen = freq_weights[:, None] / (1.0 + 4.0 * offset * offset)

        def screen_of(row_at, r_at):
            return lax.dynamic_slice_in_dim(screen, (row_at * R + r_at) * bands, bands, 1)

        right = jnp.concatenate([screen_of(row, (r + o) % R) for o in range(R)], axis=1)
        parts = {}
        for j in reversed(range(A)):
            block = turned[j]
            left = jnp.stack([block, jnp.stack([-block[1], block[0]])])
            pairs = jnp.einsum(
                "dcnk,wcmk->wdnm", left, applied, preferred_element_type=jnp.float32
            )
            factor = 0.5 * (screen_of(a ^ j, r)[:, :, None] + right[:, None, :])
            parts[j] = jnp.sum(pairs * factor[:, None], axis=0)
        bit = 1
        while bit < A:
            wire = jnp.float32 if bit < high else jnp.bfloat16
            kept = [j for j in parts if not j & bit]
            sent = jnp.stack([parts[j | bit].astype(wire) for j in kept])
            got = move(sent, flip(bit)).astype(jnp.float32)
            parts = {j: parts[j] + got[i] for i, j in enumerate(kept)}
            bit *= 2
        total = move(parts[0].astype(jnp.bfloat16), transpose).astype(jnp.float32)
        cut = jnp.split(total, R, axis=2)
        if R == 1:
            return total
        cut = jnp.stack(cut)
        return jnp.concatenate(
            [lax.dynamic_index_in_dim(cut, (j - r) % R, 0, keepdims=False) for j in range(R)], axis=2
        )

    return on_device


def solution(mesh):
    placed = (P(None, "band", "ga"), P(None, None, "ga", None), P(), P(), P(), P())
    A = mesh.shape["ga"]
    body = build(mesh.shape["band"], A)

    return jax.shard_map(
        body, mesh=mesh, in_specs=placed, out_specs=P(None, "band", "ga"), check_vma=False
    )
```
